32 devices in a mesh: pix: 4 (over x, core), frm: 8 (over z, y).
Axes of the slice: x: 2, y: 2, z: 4, core: 2. Of those that a mesh axis runs over, the one named last changes fastest.
Arguments:
- movie: bfloat16 [2048, 2048], P('pix', 'frm'), may hold values from -6 to 6
- taps: float32 [257], replicated, may hold values from -0.25 to 0.25
- scale: float32 [2048], P('pix'), may hold values from 0.3 to 3
- base: float32 [2048], P('pix'), may hold values from 0.2 to 1.5
- spatial: float32 [2048, 256], P('pix'), may hold values from 0.005 to 2
- temporal: float32 [256, 2048], P(None, 'frm'), may hold values from 0.01 to 1.1
Outputs:
- spatial_out: float32 [2048, 256], P('pix')
- temporal_out: float32 [256, 2048], P(None, 'frm')
The draws below stay inside these ranges and needn't reach their ends.
All inputs are finite; a program needn't handle non-finite values.
Results may differ from the reference program's by a relative error of at most 0.0023.
Values may be sent and summed in bfloat16 or wider, within the bound.
No kernel may reach another device: no remote copies, remote signals or barrier semaphores. Data moves between devices by JAX's collectives and lax.ppermute only.
A program may use at most 64 MiB of HBM per device.

```python
import math
import jax
import jax.numpy as jnp
from jax import lax

NUM_COMPONENTS = 256
TAPS = 257
ROUNDS = 2
PIXELS = 2048
FRAME_TOTAL = 2048


def geometric_draw(key, shape, lower, upper):
    return jnp.exp(jax.random.uniform(key, shape, jnp.float32, jnp.log(lower), jnp.log(upper)))


def planted(key):
    offset_seed = jax.random.fold_in(key, 101)
    member_key = jax.random.fold_in(offset_seed, 1)
    amplitude_key = jax.random.fold_in(offset_seed, 2)
    activity_seed = jax.random.fold_in(offset_seed, 3)
    const_key = jax.random.fold_in(offset_seed, 4)
    spike_train_key = jax.random.fold_in(offset_seed, 5)
    height_key = jax.random.fold_in(offset_seed, 6)
    starting_key = jax.random.fold_in(offset_seed, 7)
    chance = min(1.0, 4.0 / NUM_COMPONENTS)
    member = jax.random.uniform(member_key, (PIXELS, NUM_COMPONENTS), jnp.float32) < chance
    amplitude = geometric_draw(amplitude_key, (PIXELS, NUM_COMPONENTS), 0.3, 1.2)
    footprint = jnp.where(member, amplitude, 0.0).astype(jnp.float32)
    mean_activity = geometric_draw(activity_seed, (NUM_COMPONENTS, 1), 0.003, 0.03)
    decay_constant = geometric_draw(const_key, (NUM_COMPONENTS, 1), 5.0, 60.0)
    spike_events = jax.random.uniform(spike_train_key, (NUM_COMPONENTS, FRAME_TOTAL), jnp.float32) < mean_activity
    pulse_sizes = jax.random.uniform(height_key, (NUM_COMPONENTS, FRAME_TOTAL), jnp.float32, 0.5, 1.5)
    spikes = jnp.where(spike_events, pulse_sizes, 0.0).astype(jnp.float32)
    decays = jnp.exp(-1.0 / decay_constant[:, 0])
    starting_level = jax.random.uniform(starting_key, (NUM_COMPONENTS,), jnp.float32, 0.0, 1.0) * mean_activity[:, 0] * decay_constant[:, 0]

    def advance(carried, column):
        updated = decays * carried + column
        return (updated, updated)
    unused, result_pixels = lax.scan(advance, starting_level, spikes.T)
    traces = result_pixels.T
    peaks = jnp.maximum(jnp.max(traces, axis=1, keepdims=True), 0.5)
    return (footprint, traces / peaks)


def draw_movie(key, part):
    footprint, traces = planted(key)
    signal = jnp.dot(footprint, traces, precision=lax.Precision.HIGHEST)
    noise_key = jax.random.fold_in(key, 202)
    noise = 0.3 * jax.random.normal(noise_key, (PIXELS, FRAME_TOTAL), jnp.float32)
    return jnp.clip(signal + noise, -6.0, 6.0).astype(jnp.bfloat16)


def draw_spatial(key, part):
    footprint, traces = planted(key)
    perturb_key = jax.random.fold_in(key, 303)
    floor_key = jax.random.fold_in(key, 304)
    perturb = geometric_draw(perturb_key, (PIXELS, NUM_COMPONENTS), 0.6, 1.4)
    floors = geometric_draw(floor_key, (PIXELS, NUM_COMPONENTS), 0.005, 0.05)
    return (footprint * perturb + floors).astype(jnp.float32)


def draw_temporal(key, part):
    footprint, traces = planted(key)
    perturb_key = jax.random.fold_in(key, 403)
    floor_key = jax.random.fold_in(key, 404)
    perturb = geometric_draw(perturb_key, (NUM_COMPONENTS, FRAME_TOTAL), 0.6, 1.4)
    floors = geometric_draw(floor_key, (NUM_COMPONENTS, FRAME_TOTAL), 0.01, 0.1)
    return (0.7 * traces * perturb + floors).astype(jnp.float32)


def block_scale(own_key, shape, pieces, smallest, largest):
    loudness, own = 1.0, jax.random.fold_in(own_key, 6)
    for axis_at, parts in pieces:
        heights = jnp.exp(jax.random.uniform(jax.random.fold_in(own, axis_at), (parts,), jnp.float32, smallest / len(pieces), largest / len(pieces)))
        loudness = loudness * jnp.repeat(heights, shape[axis_at] // parts).reshape([-1 if axis == axis_at else 1 for axis in range(len(shape))])
    return loudness


def gaussian(rng, shape, scale, most, kind=jnp.bfloat16):
    entries = scale * jax.random.normal(rng, shape, jnp.float32)
    return jnp.clip(entries, min=-most, max=most).astype(kind)


def setup_inputs(seed: int = 0) -> dict:
    key_list = jax.random.split(jax.random.key(seed), 7)
    movie = draw_movie(jax.random.fold_in(key_list[6], 71), 0)
    taps = gaussian(key_list[1], (TAPS,), 0.0625, 0.25, jnp.float32)
    scale = jnp.clip(jnp.exp(math.log(3.0) - 2.3025851 * jax.random.uniform(key_list[2], (PIXELS,), jnp.float32) ** block_scale(key_list[2], (PIXELS,), ((0, 4),), -0.2, 0.2)), 0.3, 3.0)
    base = jnp.clip(0.2 + 1.3 * jax.random.uniform(key_list[3], (PIXELS,), jnp.float32) ** block_scale(key_list[3], (PIXELS,), ((0, 4),), -0.2, 0.2), 0.2, 1.5)
    spatial = draw_spatial(jax.random.fold_in(key_list[6], 71), 0)
    temporal = draw_temporal(jax.random.fold_in(key_list[6], 71), 0)
    return {"movie": movie, "taps": taps, "scale": scale, "base": base, "spatial": spatial, "temporal": temporal}


epsilon = 1e-6


def band_matrix(taps, block_len):
    width = taps.shape[0]
    half_width = (width - 1) // 2
    delta = jnp.where(jnp.arange(width, dtype=jnp.int32) == half_width, 1.0, 0.0).astype(jnp.float32)
    coefs = delta - taps
    period = width + block_len
    padded_row = jnp.concatenate([coefs, jnp.zeros((block_len,), jnp.float32)])
    tiled = jnp.tile(padded_row, block_len)
    skewed = tiled[: block_len * (period - 1)].reshape(block_len, period - 1)
    return skewed.T.astype(jnp.bfloat16)


def detrend(padded, taps, scale, base, frame_count):
    half_width = (taps.shape[0] - 1) // 2
    block_len = min(frame_count, 256)
    band = band_matrix(taps, block_len)
    pixel_count = padded.shape[0]

    def one_block(block_id):
        window = lax.dynamic_slice_in_dim(padded, block_id * block_len, block_len + 2 * half_width, 1)
        mixed = jnp.dot(window, band, preferred_element_type=jnp.float32)
        return jnp.maximum(scale[:, None] * mixed + base[:, None], 0.0).astype(jnp.bfloat16)

    blocks = lax.map(one_block, jnp.arange(frame_count // block_len, dtype=jnp.int32))
    return jnp.transpose(blocks, (1, 0, 2)).reshape(pixel_count, frame_count)


def reference(movie, taps, scale, base, spatial, temporal):
    half_width = (taps.shape[0] - 1) // 2
    frame_count = movie.shape[1]
    padded = jnp.pad(movie, ((0, 0), (half_width, half_width)))
    normalised = detrend(padded, taps, scale, base, frame_count)
    spatial_now = spatial
    temporal_now = temporal
    for round_id in range(ROUNDS):
        temporal_copy = temporal_now.astype(jnp.bfloat16)
        numer = jnp.dot(normalised, temporal_copy.T, preferred_element_type=jnp.float32)
        gram = jnp.dot(temporal_now, temporal_now.T, precision=lax.Precision.HIGHEST)
        spatial_now = spatial_now * numer / (jnp.dot(spatial_now, gram, precision=lax.Precision.HIGHEST) + epsilon)
        spatial_copy = spatial_now.astype(jnp.bfloat16)
        numer_t = lax.dot_general(spatial_copy, normalised, (((0,), (0,)), ((), ())), preferred_element_type=jnp.float32)
        gram_t = lax.dot_general(spatial_now, spatial_now, (((0,), (0,)), ((), ())), precision=lax.Precision.HIGHEST)
        temporal_now = temporal_now * numer_t / (jnp.dot(gram_t, temporal_now, precision=lax.Precision.HIGHEST) + epsilon)
    return spatial_now, temporal_now
```

```python
import jax
import jax.numpy as jnp
from jax import lax
from jax.sharding import PartitionSpec as P

ROUNDS = 2


epsilon = 1e-06

f32, bf16 = jnp.float32, jnp.bfloat16


def band_matrix(taps, block_len):
    width = taps.shape[0]
    half_width = (width - 1) // 2
    delta = jnp.where(jnp.arange(width, dtype=jnp.int32) == half_width, 1.0, 0.0).astype(f32)
    coefs = delta - taps
    period = width + block_len
    padded_row = jnp.concatenate([coefs, jnp.zeros((block_len,), f32)])
    tiled = jnp.tile(padded_row, block_len)
    skewed = tiled[: block_len * (period - 1)].reshape(block_len, period - 1)
    return skewed.T.astype(bf16)


def matmul(a, b):
    return jnp.dot(a, b, preferred_element_type=f32)


def matmul_t(a, b):
    return lax.dot_general(a, b, (((1,), (1,)), ((), ())), preferred_element_type=f32)


def t_matmul(a, b):
    return lax.dot_general(a, b, (((0,), (0,)), ((), ())), preferred_element_type=f32)


def swap(value, axis, mask):
    size = lax.axis_size(axis)
    return lax.ppermute(value, axis, [(i, i ^ mask) for i in range(size)])


def halos(movie, width):
    size, length = lax.axis_size("frm"), movie.shape[1]
    up = [(i, i + 1) for i in range(size - 1)]
    down = [(j, i) for i, j in up]
    before = lax.ppermute(movie[:, length - width :], "frm", up)
    after = lax.ppermute(movie[:, :width], "frm", down)
    return before, after


def reorder(value, index, parts, dim):
    bit = 1
    while bit < parts:
        blocks = jnp.split(value, parts, axis=dim)
        other = jnp.concatenate([blocks[b ^ bit] for b in range(parts)], axis=dim)
        value = jnp.where((index & bit) != 0, other, value)
        bit *= 2
    return value


def on_device(movie, taps, scale, base, spatial, temporal):
    half_width = (taps.shape[0] - 1) // 2
    pixels, frames = movie.shape
    n_frm, n_pix = lax.axis_size("frm"), lax.axis_size("pix")
    quad, pair = min(4, n_frm), min(2, n_pix)
    rows, cols = pixels // quad, frames // pair
    me_frm, me_pix = lax.axis_index("frm") % quad, lax.axis_index("pix") % pair

    before, after = halos(movie, half_width)
    band = band_matrix(taps, frames)
    padded = jnp.concatenate([before, movie, after], axis=1)
    mixed = matmul(padded, band)
    normalised = jnp.maximum(scale[:, None] * mixed + base[:, None], 0.0).astype(bf16)
    normalised = reorder(reorder(normalised, me_frm, quad, 0), me_pix, pair, 1)
    spatial = reorder(spatial, me_frm, quad, 0)
    temporal = reorder(temporal, me_pix, pair, 1)

    spatial_own = spatial[:rows]
    spatial_copy = spatial.astype(bf16)
    temporal_own = temporal[:, :cols]
    for round_id in range(ROUNDS):
        last = round_id == ROUNDS - 1
        temporal_copy = temporal.astype(bf16)
        model = matmul(spatial_copy, temporal_copy).astype(bf16)
        numer = matmul_t(normalised, temporal_copy)
        denom = matmul_t(model, temporal_copy)
        part = jnp.stack([numer.reshape(quad, rows, -1), denom.reshape(quad, rows, -1)], 1)
        total = part[0]
        for mask in range(1, quad):
            total = total + swap(part[mask].astype(bf16), "frm", mask).astype(f32)
        rough, mask = total, quad
        while mask < n_frm:
            high = rough.astype(bf16)
            low = (total - high.astype(f32)).astype(bf16)
            high_in, low_in = swap(high, "frm", mask), swap(low, "frm", mask)
            rough = high.astype(f32) + high_in.astype(f32)
            total = rough + (low.astype(f32) + low_in.astype(f32))
            mask *= 2
        copy_own = (spatial_own * rough[0] / (rough[1] + epsilon)).astype(bf16)
        spatial_own = spatial_own * total[0] / (total[1] + epsilon)
        spatial_copy = jnp.concatenate(
            [copy_own] + [swap(copy_own, "frm", mask) for mask in range(1, quad)], axis=0
        )
        model = matmul(spatial_copy, temporal_copy).astype(bf16)
        numer = t_matmul(spatial_copy, normalised)
        denom = t_matmul(spatial_copy, model)
        total = jnp.stack([numer[:, :cols], denom[:, :cols]])
        if pair > 1:
            total = total + swap(jnp.stack([numer[:, cols:], denom[:, cols:]]), "pix", 1)
        mask = pair
        while mask < n_pix:
            total = total + swap(total, "pix", mask)
            mask *= 2
        temporal_own = temporal_own * total[0] / (total[1] + epsilon)
        temporal = temporal_own
        if pair > 1:
            temporal = jnp.concatenate([temporal_own, swap(temporal_own, "pix", 1)], axis=1)

    spatial = jnp.concatenate(
        [spatial_own] + [swap(spatial_own, "frm", mask) for mask in range(1, quad)], axis=0
    )
    return reorder(spatial, me_frm, quad, 0), reorder(temporal, me_pix, pair, 1)


def solution(mesh):
    placed = (P("pix", "frm"), P(), P("pix"), P("pix"), P("pix", None), P(None, "frm"))
    return jax.shard_map(
        on_device,
        mesh=mesh,
        in_specs=placed,
        out_specs=(P("pix", None), P(None, "frm")),
        check_vma=False,
    )
```
